32 devices in a mesh: sa: 4 (over y, core), sb: 8 (over z, x).
Axes of the slice: x: 2, y: 2, z: 4, core: 2. Of those that a mesh axis runs over, the one named last changes fastest.
Arguments:
- queries: bfloat16 [1024, 1024], P(('sa', 'sb')), may hold values from -6 to 6
- out_grad: bfloat16 [1024, 1024], P(('sa', 'sb')), may hold values from -6144 to 6144
- forward_out: bfloat16 [1024, 1024], P(('sa', 'sb')), may hold values from -3 to 3
- lse_shift: float32 [1024, 8], P(('sa', 'sb')), may hold values from 0.2 to 1
- key_rows: bfloat16 [32768, 256], P(('sa', 'sb')), may hold values from -7 to 7
- value_rows: bfloat16 [32768, 256], P(('sa', 'sb')), may hold values from -6 to 6
Outputs:
- query_grad: float32 [1024, 1024], P(('sa', 'sb'))
- key_grad: bfloat16 [32768, 256], P(('sa', 'sb'))
- value_grad: bfloat16 [32768, 256], P(('sa', 'sb'))
The draws below stay inside these ranges and needn't reach their ends.
All inputs are finite; a program needn't handle non-finite values.
Results may differ from the reference program's by a relative error of at most 0.0097.
Values may be sent and summed in bfloat16 or wider, within the bound.
A program may use at most 64 MiB of HBM per device.

```python
import math
import jax
import jax.numpy as jnp
from jax import lax

QH = 8
KVH = 2
HEAD_DIM = 128
Q_ROWS = 1024
KEYS = 32768


def draw_key_rows(key, part):
    noise_key, offset_key = jax.random.split(jax.random.fold_in(key, 11))
    noise = jnp.clip(jax.random.normal(noise_key, (KEYS, KVH * HEAD_DIM), jnp.float32), -4.0, 4.0)
    offset = jax.random.uniform(offset_key, (KVH * HEAD_DIM,), jnp.float32, -1.0, 1.0)
    ramp = 1.0 + 2.0 * jnp.arange(KEYS, dtype=jnp.float32) / KEYS
    return (noise + ramp[:, None] * offset[None, :]).astype(jnp.bfloat16)


def levels(key, extent, shards, low, high):
    def one(axis_at, shards_of):
        draws = jax.random.uniform(jax.random.fold_in(jax.random.fold_in(key, 6), axis_at), (shards_of,), jnp.float32, low / len(shards), high / len(shards))
        return jnp.repeat(jnp.exp(draws), extent[axis_at] // shards_of).reshape((-1,) + (1,) * (len(extent) - axis_at - 1))

    factor_of = one(*shards[0])
    for cut in shards[1:]:
        factor_of = factor_of * one(*cut)
    return factor_of


def scatter_about(stream_key, dims, scale, bound, cuts=(), held_as=jnp.bfloat16):
    result = jax.random.normal(stream_key, dims, jnp.float32) * scale
    if len(cuts) > 0:
        result = levels(stream_key, dims, cuts, -0.22, 0.18) * result
    return jnp.clip(result, min=-bound, max=bound).astype(held_as)


def setup_inputs(seed: int = 0) -> dict:
    streams_of = jax.random.split(jax.random.key(seed), 7)
    return {
        "queries": scatter_about(streams_of[0], (Q_ROWS, QH * HEAD_DIM), 1.0, 6.0, ((0, 32),)),
        "out_grad": scatter_about(streams_of[1], (Q_ROWS, QH * HEAD_DIM), 1024.0, 6144.0, ((0, 32),)),
        "forward_out": scatter_about(streams_of[2], (Q_ROWS, QH * HEAD_DIM), 0.5, 3.0, ((0, 32),)),
        "lse_shift": jnp.clip(0.2 + 0.8 * jax.random.uniform(streams_of[3], (Q_ROWS, QH), jnp.float32) ** levels(streams_of[3], (Q_ROWS, QH), ((0, 32),), -0.2, 0.2), 0.2, 1.0),
        "key_rows": draw_key_rows(jax.random.fold_in(streams_of[6], 71), 0),
        "value_rows": scatter_about(streams_of[5], (KEYS, KVH * HEAD_DIM), 1.0, 6.0, ((0, 32),)),
    }


def reference(queries, out_grad, forward_out, lse_shift, key_rows, value_rows):
    per_group = QH // KVH
    score_scale = 1.0 / math.sqrt(HEAD_DIM)
    key_mean = lax.optimization_barrier(jnp.sum(key_rows.astype(jnp.float32), axis=0)) / KEYS
    smoothed = (key_rows.astype(jnp.float32) - key_mean).astype(jnp.bfloat16)
    query_full = queries.astype(jnp.float32).reshape(Q_ROWS, KVH, per_group, HEAD_DIM)
    grad_full = out_grad.astype(jnp.float32).reshape(Q_ROWS, KVH, per_group, HEAD_DIM)
    product = out_grad.astype(jnp.float32) * forward_out.astype(jnp.float32)
    delta_rows = lax.optimization_barrier(jnp.sum(product.reshape(Q_ROWS, QH, HEAD_DIM), axis=-1))
    delta_heads = delta_rows.reshape(Q_ROWS, KVH, per_group).transpose(1, 2, 0)[..., None]
    offset_rows = lse_shift + math.log(KEYS)
    offset_heads = offset_rows.reshape(Q_ROWS, KVH, per_group).transpose(1, 2, 0)[..., None]
    key_block = 4096 if KEYS % 4096 == 0 else KEYS
    blocks = KEYS // key_block
    key_blocks = smoothed.reshape(blocks, key_block, KVH, HEAD_DIM)
    value_blocks = value_rows.reshape(blocks, key_block, KVH, HEAD_DIM)

    def block_step(query_acc, pieces):
        key_part = pieces[0].astype(jnp.float32)
        value_part = pieces[1].astype(jnp.float32)
        scores = jnp.einsum('qcgd,kcd->cgqk', query_full, key_part) * score_scale
        prob = jnp.exp(scores - offset_heads)
        prob_low = lax.optimization_barrier(prob.astype(jnp.bfloat16)).astype(jnp.float32)
        value_part_grad = jnp.einsum('cgqk,qcgd->kcd', prob_low, grad_full)
        dprob = jnp.einsum('qcgd,kcd->cgqk', grad_full, value_part)
        dscore = lax.optimization_barrier((prob * (dprob - delta_heads)).astype(jnp.bfloat16)).astype(jnp.float32)
        key_part_grad = jnp.einsum('cgqk,qcgd->kcd', dscore, query_full) * score_scale
        query_acc = query_acc + jnp.einsum('cgqk,kcd->qcgd', dscore, key_part) * score_scale
        return (query_acc, (key_part_grad.astype(jnp.bfloat16), value_part_grad.astype(jnp.bfloat16)))
    start = jnp.zeros((Q_ROWS, KVH, per_group, HEAD_DIM), jnp.float32)
    query_acc, outputs = lax.scan(block_step, start, (key_blocks, value_blocks))
    key_grad = outputs[0].reshape(KEYS, KVH * HEAD_DIM)
    value_grad = outputs[1].reshape(KEYS, KVH * HEAD_DIM)
    return (query_acc.reshape(Q_ROWS, QH * HEAD_DIM), key_grad, value_grad)
```

```python
import functools
import math

import jax
import jax.numpy as jnp
from jax import lax
from jax.experimental import pallas as pl
from jax.experimental.pallas import tpu as pltpu
from jax.sharding import PartitionSpec as P

QH = 8
KVH = 2
HEAD_DIM = 128
MESH = pl.DeviceIdType.MESH
BF = jnp.bfloat16
F32 = jnp.float32
AXES = ("sa", "sb")


def grid_of(sa, sb):
    inner = 2 ** (int(math.log2(sb)) // 2)
    return sa // 2, sb // inner, inner


class Place:
    def __init__(self, dims):
        self.dims = dims
        sa, sb = lax.axis_index("sa"), lax.axis_index("sb")
        self.core = sa % 2
        self.at = (sa // 2, sb // dims[2], sb % dims[2])

    def other(self, axis, step):
        at = list(self.at)
        at[axis] = (at[axis] + step) % self.dims[axis]
        return tuple(at)

    def back(self, offset):
        return tuple((p + n - o) % n for p, n, o in zip(self.at, self.dims, offset))

    def device(self, at):
        return (at[0] * 2 + self.core, at[1] * self.dims[2] + at[2])

    def partner(self):
        return (self.at[0] * 2 + 1 - self.core, lax.axis_index("sb"))

    def slot(self, at):
        return (at[0] * self.dims[1] + at[1]) * self.dims[2] + at[2]

    def greet(self):
        barrier = pltpu.get_barrier_semaphore()
        peers = [self.partner()]
        for axis in range(3):
            for step in range(1, self.dims[axis]):
                peers.append(self.device(self.other(axis, step)))
        for peer in peers:
            pl.semaphore_signal(barrier, inc=1, device_id=peer, device_id_type=MESH)
        pl.semaphore_wait(barrier, len(peers))


def pieces(x):
    hi = x.astype(BF)
    rest = x - hi.astype(F32)
    mid = rest.astype(BF)
    low = (rest - mid.astype(F32)).astype(BF)
    return hi, mid, low


def relay_lines(dims, b):
    na, nb, nd = dims
    sends = [((0, b, 0), 2, step) for step in range(1, nd)]
    return sends + [((0, b, 0), 0, step) for step in range(1, na)]


def relay_corners(dims, b):
    na, nb, nd = dims
    sends = [("q", (0, b, d), 0, s) for d in range(1, nd) for s in range(1, na)]
    return sends + [("d", (a, b, 0), 2, s) for a in range(1, na) for s in range(1, nd)]


def first_sends(dims):
    along = [(1, step) for step in range(1, dims[1])]
    across = [(2, step) for step in range(1, dims[2])] + [(0, step) for step in range(1, dims[0])]
    return along, across


def line_order(dims):
    lines = [(a, d) for a in range(dims[0]) for d in range(dims[2])]
    return sorted(lines, key=lambda at: (at[0] != 0) + (at[1] != 0))


def counts(dims):
    na, nb, nd = dims
    along, across = first_sends(dims)
    gathered = 4 * (len(along) + len(across))
    for b in range(nb):
        gathered += 2 * KVH * len(relay_lines(dims, b)) * (b > 0) + KVH * len(relay_corners(dims, b))
    lines = line_order(dims)
    reduced = sum((a != 0) + (d != 0) for a, d in lines) + (na - 1) + (nd - 1) + (nb - 1)
    return gathered, KVH * reduced, (nb - 1) + (nd - 1) + (na - 1)


def whole_kernel(dims, total_keys, tile, q_ref, d_ref, o_ref, lse_ref, k_ref, v_ref,
                 dq_out, dk_out, dv_out,
                 qa, da0, da1, kt, vt, ksend, krecv, auxs, qts, dts, ps, dss, dqs,
                 dk_acc, dv_acc, part, kvs, kvr,
                 r1a, r1b, t1a, t1b, r2a, r2b, t2, r3,
                 send_sem, q_sem, d_sem, kv_send, kv_recv, sum_send, sum_recv,
                 red_send, r1a_sem, r1b_sem, r2a_sem, r2b_sem, r3_sem):
    na, nb, nd = dims
    place = Place(dims)
    pa, pb, pd = place.at
    rows = q_ref.shape[0]
    keys = k_ref.shape[0]
    group = q_ref.shape[1] // KVH
    per_group = QH // KVH
    scale = 1.0 / math.sqrt(HEAD_DIM)
    along, across = first_sends(dims)
    origin = (0, 0, 0)
    block = nb * rows
    cols = block * per_group

    lane = lax.broadcasted_iota(jnp.int32, (rows, HEAD_DIM), 1)
    lse_rows = lse_ref[...].T
    aux = jnp.zeros((rows, HEAD_DIM), F32)
    for head in range(QH):
        at = pl.ds(head * HEAD_DIM, HEAD_DIM)
        product = d_ref[:, at].astype(F32) * o_ref[:, at].astype(F32)
        delta = jnp.sum(product, axis=1, keepdims=True)
        offset = (lse_rows[:, head:head + 1] + math.log(total_keys)) * (1.0 / scale)
        for first, value in ((0, offset), (3 * QH, delta)):
            for n, piece in enumerate(pieces(value)):
                aux = jnp.where(lane == first + 3 * head + n, piece.astype(F32), aux)
    da0[pa, pb, pd, :, pl.ds(group, HEAD_DIM)] = aux.astype(BF)
    da0[pa, pb, pd, :, pl.ds(0, group)] = d_ref[:, pl.ds(0, group)]
    da1[pa, pb, pd] = d_ref[:, pl.ds(group, group)]
    for c in range(KVH):
        qa[c, pa, pb, pd] = q_ref[:, pl.ds(c * group, group)]
    chunk = 128

    def turn(n, total):
        at = pl.ds(pl.multiple_of(n * chunk, chunk), chunk)
        for c in range(KVH):
            head = pl.ds(c * HEAD_DIM, HEAD_DIM)
            kt[0, c, :, at] = k_ref[at, head].T
            vt[0, c, :, at] = v_ref[at, head].T
        return total + jnp.sum(k_ref[at, :].astype(F32), axis=0, keepdims=True)

    key_sum = lax.fori_loop(0, keys // chunk, turn, jnp.zeros((1, KVH * HEAD_DIM), F32))
    row8 = lax.broadcasted_iota(jnp.int32, (8, HEAD_DIM), 0)
    sums = jnp.zeros((8, HEAD_DIM), F32)
    for c in range(KVH):
        sums = jnp.where(row8 == c, key_sum[:, c * HEAD_DIM:(c + 1) * HEAD_DIM], sums)
    ksend[0] = sums

    place.greet()

    partner_copies = []

    def to_partner(src, dst):
        n = len(partner_copies)
        copy = pltpu.make_async_remote_copy(
            src_ref=src, dst_ref=dst, send_sem=kv_send.at[n], recv_sem=kv_recv.at[n],
            device_id=place.partner(), device_id_type=MESH)
        copy.start()
        partner_copies.append(copy)
        return copy

    sum_copies = []

    def send_sums(stage, axis):
        group_of = []
        for step in range(1, dims[axis]):
            n = len(sum_copies)
            copy = pltpu.make_async_remote_copy(
                src_ref=ksend.at[stage], dst_ref=krecv.at[n],
                send_sem=sum_send.at[n], recv_sem=sum_recv.at[n],
                device_id=place.device(place.other(axis, step)), device_id_type=MESH)
            copy.start()
            sum_copies.append(copy)
            group_of.append((copy, n))
        return group_of

    def add_sums(stage, group_of):
        total = ksend[stage]
        for copy, n in group_of:
            copy.wait_recv()
            total = total + krecv[n]
        ksend[stage + 1] = total

    def flat(offset):
        return (offset[0] * nb + offset[1]) * nd + offset[2]

    def places(kind, at, offset):
        c = int(kind[1])
        if kind[0] == "q":
            return qa.at[c, at[0], at[1], at[2]], q_sem.at[c, flat(offset)]
        return (da0, da1)[c].at[at[0], at[1], at[2]], d_sem.at[c, flat(offset)]

    started = []

    def send(kind, offset, axis, step):
        there = list(offset)
        there[axis] = (there[axis] + step) % dims[axis]
        ref, sem = places(kind, place.back(offset), there)
        copy = pltpu.make_async_remote_copy(
            src_ref=ref, dst_ref=ref, send_sem=send_sem.at[len(started)], recv_sem=sem,
            device_id=place.device(place.other(axis, step)), device_id_type=MESH)
        copy.start()
        started.append(copy)

    arrived = set()

    def need(kind, offset):
        if offset == origin or (kind, offset) in arrived:
            return
        arrived.add((kind, offset))
        ref, sem = places(kind, place.back(offset), offset)
        pltpu.make_async_remote_copy(
            src_ref=ref, dst_ref=ref, send_sem=send_sem.at[0], recv_sem=sem,
            device_id=place.partner(), device_id_type=MESH).wait_recv()

    def send_first(c, directions):
        for kind in ("q", "d"):
            for axis, step in directions:
                send(kind + str(c), origin, axis, step)

    def send_line(c, b):
        for kind in ("q", "d"):
            need(kind + str(c), (0, b, 0))
        for kind in ("q", "d"):
            for offset, axis, step in relay_lines(dims, b):
                send(kind + str(c), offset, axis, step)

    def send_corner(c, b):
        for kind, offset, axis, step in relay_corners(dims, b):
            need(kind + str(c), offset)
            send(kind + str(c), offset, axis, step)

    def need_line(c, a, d):
        for b in range(nb):
            for kind in ("q", "d"):
                need(kind + str(c), (a, b, d))

    stage = send_sums(0, 1)
    send_first(0, along + across)
    k_copy = to_partner(kt.at[0], kt.at[1])
    v_copy = to_partner(vt.at[0], vt.at[1])
    send_first(1, across)
    add_sums(0, stage)
    stage = send_sums(1, 2)
    send_corner(0, 0)
    if nb > 1:
        send_line(0, 1)
    add_sums(1, stage)
    stage = send_sums(2, 0)
    for b in range(2, nb):
        send_line(0, b)
    add_sums(2, stage)
    sum_copy = to_partner(ksend.at[3], ksend.at[4])
    send_first(1, along)
    k_copy.wait_recv()
    v_copy.wait_recv()
    sum_copy.wait_recv()
    k_copy.wait_send()
    mean = (ksend[3] + ksend[4]) * (1.0 / total_keys)
    means = []
    for c in range(KVH):
        means.append(jnp.broadcast_to(mean[c:c + 1], (HEAD_DIM, HEAD_DIM)).T)

    def smooth(n, carry):
        at = pl.ds(pl.multiple_of(n * chunk, chunk), chunk)
        for side in range(2):
            for c in range(KVH):
                kt[side, c, :, at] = (kt[side, c, :, at].astype(F32) - means[c]).astype(BF)
        return carry

    lax.fori_loop(0, keys // chunk, smooth, 0)

    nt = (((1,), (1,)), ((), ()))
    tiles = keys // tile
    lane_b = lax.broadcasted_iota(jnp.int32, (block, HEAD_DIM), 1)

    def line_at(a, d):
        return (pa + na - a) % na, (pd + nd - d) % nd

    def prepare(n, c, a, d):
        la, ld = line_at(a, d)
        aux_rows = da0[la, :, ld, :, pl.ds(group, HEAD_DIM)].reshape(block, HEAD_DIM)
        for g in range(per_group):
            head = pl.ds(g * HEAD_DIM, HEAD_DIM)
            here = pl.ds(g * block, block)
            low = 3 * (c * per_group + g)
            keep = (lane_b >= low) & (lane_b < low + 3)
            low = low + 3 * QH
            keep = keep | ((lane_b >= low) & (lane_b < low + 3))
            auxs[n, here, :] = jnp.where(keep, aux_rows.astype(F32), 0.0).astype(BF)
            qts[n, :, here] = qa[c, la, :, ld, :, head].reshape(block, HEAD_DIM).T
            dts[n, :, here] = (da0, da1)[c][la, :, ld, :, head].reshape(block, HEAD_DIM).T

    def scores(n, m, c, a, d, side, t):
        la, ld = line_at(a, d)
        at = pl.ds(t * tile, tile)
        key_row = lax.broadcasted_iota(jnp.int32, (HEAD_DIM, tile), 0)
        pick_s = jnp.where(key_row < 3 * QH, -1.0, 0.0).astype(BF)
        pick_d = jnp.where((key_row >= 3 * QH) & (key_row < 6 * QH), -1.0, 0.0).astype(BF)
        kk = jnp.concatenate([kt[side, c, :, at], pick_s], 0)
        vv = jnp.concatenate([vt[side, c, :, at], pick_d], 0)
        for g in range(per_group):
            head = pl.ds(g * HEAD_DIM, HEAD_DIM)
            here = pl.ds(g * block, block)
            qh = qa[c, la, :, ld, :, head].reshape(block, HEAD_DIM)
            dh = (da0, da1)[c][la, :, ld, :, head].reshape(block, HEAD_DIM)
            s = jnp.dot(jnp.concatenate([qh, auxs[n, here, :]], 1), kk, preferred_element_type=F32)
            dp = jnp.dot(jnp.concatenate([dh, auxs[n, here, :]], 1), vv, preferred_element_type=F32)
            prob = jnp.exp2(s * (scale * math.log2(math.e)))
            ps[m, here, :] = prob.astype(BF)
            dss[m, here, :] = (prob * dp).astype(BF)

    def products(n, m, c, side, t, first_line, first_tile):
        at = pl.ds(t * tile, tile)
        dv = jnp.dot(dts[n], ps[m], preferred_element_type=F32)
        dk = jnp.dot(qts[n], dss[m], preferred_element_type=F32)
        dq = lax.dot_general(kt[side, c, :, at], dss[m], nt, preferred_element_type=F32)
        if first_line:
            dv_acc[side, c, :, at] = dv
            dk_acc[side, c, :, at] = dk
        else:
            dv_acc[side, c, :, at] += dv
            dk_acc[side, c, :, at] += dk
        if first_tile:
            dqs[n] = dq
        else:
            dqs[n] += dq

    def finish(n, c, a, d):
        la, ld = line_at(a, d)
        for g in range(per_group):
            here = pl.ds(g * block, block)
            piece = (dqs[n, :, here] * scale).astype(BF).T
            part[c, la, :, ld, :, pl.ds(g * HEAD_DIM, HEAD_DIM)] = piece.reshape(nb, rows, HEAD_DIM)

    mid = group // 2
    left, right = pl.ds(0, mid), pl.ds(mid, mid)
    reduced = []

    def red(src, dst, sem, to):
        copy = pltpu.make_async_remote_copy(
            src_ref=src, dst_ref=dst, send_sem=red_send.at[len(reduced)], recv_sem=sem,
            device_id=place.device(to), device_id_type=MESH)
        copy.start()
        reduced.append(copy)

    def landed(ref, sem):
        pltpu.make_async_remote_copy(
            src_ref=ref, dst_ref=ref, send_sem=red_send.at[0], recv_sem=sem,
            device_id=place.partner(), device_id_type=MESH).wait_recv()

    def stage1(c, a, d):
        la, ld = line_at(a, d)
        if d:
            s = nd - d
            red(part.at[c, la, :, ld, :, left], r1a.at[c, s - 1, la],
                r1a_sem.at[c, s - 1, a], place.other(2, s))
        if a:
            s = na - a
            red(part.at[c, la, :, ld, :, right], r1b.at[c, s - 1, ld],
                r1b_sem.at[c, s - 1, d], place.other(0, s))

    def sum_left(c, a):
        la, _ = line_at(a, 0)
        total = part[c, la, :, pd, :, left].astype(F32)
        for s in range(nd - 1):
            landed(r1a.at[c, s, la], r1a_sem.at[c, s, a])
            total = total + r1a[c, s, la].astype(F32)
        return total

    def sum_right(c, d):
        _, ld = line_at(0, d)
        total = part[c, pa, :, ld, :, right].astype(F32)
        for s in range(na - 1):
            landed(r1b.at[c, s, ld], r1b_sem.at[c, s, d])
            total = total + r1b[c, s, ld].astype(F32)
        return total

    def stage2(c):
        for a in range(1, na):
            t1a[c, a] = sum_left(c, a).astype(BF)
            s = na - a
            red(t1a.at[c, a], r2a.at[c, s - 1], r2a_sem.at[c, s - 1], place.other(0, s))
        for d in range(1, nd):
            t1b[c, d] = sum_right(c, d).astype(BF)
            s = nd - d
            red(t1b.at[c, d], r2b.at[c, s - 1], r2b_sem.at[c, s - 1], place.other(2, s))

    def stage3(c):
        total = sum_left(c, 0)
        for s in range(na - 1):
            landed(r2a.at[c, s], r2a_sem.at[c, s])
            total = total + r2a[c, s].astype(F32)
        t2[c, :, :, left] = total.astype(BF)
        total = sum_right(c, 0)
        for s in range(nd - 1):
            landed(r2b.at[c, s], r2b_sem.at[c, s])
            total = total + r2b[c, s].astype(F32)
        t2[c, :, :, right] = total.astype(BF)
        for s in range(1, nb):
            to = place.other(1, s)
            red(t2.at[c, to[1]], r3.at[c, s - 1], r3_sem.at[c, s - 1], to)

    def last(c):
        total = t2[c, pb].astype(F32)
        for s in range(nb - 1):
            landed(r3.at[c, s], r3_sem.at[c, s])
            total = total + r3[c, s].astype(F32)
        dq_out[:, pl.ds(c * group, group)] = total

    kv = []

    def share(c):
        for which, acc, factor in ((0, dk_acc, scale), (1, dv_acc, 1.0)):
            kvs[c, which] = (acc[1, c] * factor).astype(BF)
            kv.append(to_partner(kvs.at[c, which], kvr.at[c, which]))

    def collect(c):
        head = pl.ds(c * HEAD_DIM, HEAD_DIM)
        for which, acc, factor, out in ((0, dk_acc, scale, dk_out), (1, dv_acc, 1.0, dv_out)):
            kv[2 * c + which].wait_recv()
            total = acc[0, c] * factor + kvr[c, which].astype(F32)
            out[:, head] = total.astype(BF).T

    lines = line_order(dims)
    orders = (lines, lines[1:][::-1] + lines[:1])
    events = {}

    def plan(c, n, half, action):
        events.setdefault((c, min(n, len(lines) - 1), half), []).append(action)

    for b in range(1, nb):
        plan(0, 0 if b < 2 else 1, b < 2, functools.partial(send_corner, 0, b))
        plan(0, 1, 1, functools.partial(send_line, 1, b))
    for b in range(nb):
        plan(0, 2, 1, functools.partial(send_corner, 1, b))
    plan(1, 1, 1, lambda: stage2(0))
    plan(1, 2, 1, lambda: stage3(0))
    plan(1, 3, 1, lambda: stage2(1))

    steps = [(side, t) for side in (1, 0) for t in range(tiles)]
    pending = None
    count = 0
    ended = None
    for c in range(KVH):
        for n, (a, d) in enumerate(orders[c]):
            for action in events.get((c, n, 0), []):
                action()
            need_line(c, a, d)
            if a or d:
                need_line(0, a, d)
            slot = n % 2
            prepare(slot, c, a, d)
            for i, (side, t) in enumerate(steps):
                if i == len(steps) // 2:
                    for action in events.get((c, n, 1), []):
                        action()
                scores(slot, count % 2, c, a, d, side, t)
                if pending is not None:
                    products(*pending)
                    pending = None
                if ended is not None:
                    finish(*ended)
                    stage1(*ended[1:])
                    ended = None
                pending = (slot, count % 2, c, side, t, n == 0, i == 0)
                count += 1
            ended = (slot, c, a, d)
        products(*pending)
        finish(*ended)
        pending = None
        stage1(*ended[1:])
        ended = None
        share(c)
    stage3(1)
    collect(0)
    last(0)
    collect(1)
    last(1)
    for copy in started + partner_copies[1:] + sum_copies + reduced:
        copy.wait_send()


def local(dims, q, d, o, lse, k, v):
    na, nb, nd = dims
    members = na * nb * nd
    rows, width = q.shape
    keys, kw = k.shape
    group, mid = width // KVH, width // KVH // 2
    cols = nb * rows * (QH // KVH)
    tile = min(512, keys)
    gathered, reduced, summed = counts(dims)
    vmem = pl.BlockSpec(memory_space=pltpu.VMEM)
    ma, mb, md = max(na - 1, 1), max(nb - 1, 1), max(nd - 1, 1)
    sem = pltpu.SemaphoreType.DMA
    return pl.pallas_call(
        functools.partial(whole_kernel, dims, keys * members * 2, tile),
        name="whole",
        out_shape=(
            jax.ShapeDtypeStruct((rows, width), F32),
            jax.ShapeDtypeStruct((keys, kw), BF),
            jax.ShapeDtypeStruct((keys, kw), BF),
        ),
        in_specs=[vmem] * 6,
        out_specs=(vmem,) * 3,
        scratch_shapes=[
            pltpu.VMEM((KVH, na, nb, nd, rows, group), BF),
            pltpu.VMEM((na, nb, nd, rows, group + HEAD_DIM), BF),
            pltpu.VMEM((na, nb, nd, rows, group), BF),
            pltpu.VMEM((2, KVH, HEAD_DIM, keys), BF),
            pltpu.VMEM((2, KVH, HEAD_DIM, keys), BF),
            pltpu.VMEM((5, 8, HEAD_DIM), F32),
            pltpu.VMEM((max(summed, 1), 8, HEAD_DIM), F32),
            pltpu.VMEM((2, cols, HEAD_DIM), BF),
            pltpu.VMEM((2, HEAD_DIM, cols), BF),
            pltpu.VMEM((2, HEAD_DIM, cols), BF),
            pltpu.VMEM((2, cols, tile), BF),
            pltpu.VMEM((2, cols, tile), BF),
            pltpu.VMEM((2, HEAD_DIM, cols), F32),
            pltpu.VMEM((2, KVH, HEAD_DIM, keys), F32),
            pltpu.VMEM((2, KVH, HEAD_DIM, keys), F32),
            pltpu.VMEM((KVH, na, nb, nd, rows, group), BF),
            pltpu.VMEM((KVH, 2, HEAD_DIM, keys), BF),
            pltpu.VMEM((KVH, 2, HEAD_DIM, keys), BF),
            pltpu.VMEM((KVH, md, na, nb, rows, mid), BF),
            pltpu.VMEM((KVH, ma, nd, nb, rows, mid), BF),
            pltpu.VMEM((KVH, na, nb, rows, mid), BF),
            pltpu.VMEM((KVH, nd, nb, rows, mid), BF),
            pltpu.VMEM((KVH, ma, nb, rows, mid), BF),
            pltpu.VMEM((KVH, md, nb, rows, mid), BF),
            pltpu.VMEM((KVH, nb, rows, group), BF),
            pltpu.VMEM((KVH, mb, rows, group), BF),
            sem((gathered,)),
            sem((KVH, members)),
            sem((KVH, members)),
            sem((3 + 2 * KVH,)),
            sem((3 + 2 * KVH,)),
            sem((max(summed, 1),)),
            sem((max(summed, 1),)),
            sem((reduced,)),
            sem((KVH, md, na)),
            sem((KVH, ma, nd)),
            sem((KVH, ma)),
            sem((KVH, md)),
            sem((KVH, mb)),
        ],
        compiler_params=pltpu.CompilerParams(
            collective_id=0, has_side_effects=True, vmem_limit_bytes=60 * 1024 * 1024),
    )(q, d, o, lse.T, k, v)


def solution(mesh):
    dims = grid_of(mesh.shape["sa"], mesh.shape["sb"])
    spec = P(("sa", "sb"), None)
    return jax.shard_map(functools.partial(local, dims), mesh=mesh, in_specs=(spec,) * 6,
                         out_specs=(spec,) * 3, check_vma=False)
```

```python
import functools
import math

import jax
import jax.numpy as jnp
from jax import lax
from jax.experimental import pallas as pl
from jax.experimental.pallas import tpu as pltpu
from jax.sharding import PartitionSpec as P

QH = 8
KVH = 2
HEAD_DIM = 128
MESH = pl.DeviceIdType.MESH
BF = jnp.bfloat16
F32 = jnp.float32
AXES = ("sa", "sb")


def grid_of(sa, sb):
    inner = 2 ** (int(math.log2(sb)) // 2)
    return sa // 2, sb // inner, inner


class Place:
    def __init__(self, dims):
        self.dims = dims
        sa, sb = lax.axis_index("sa"), lax.axis_index("sb")
        self.core = sa % 2
        self.at = (sa // 2, sb // dims[2], sb % dims[2])

    def other(self, axis, step):
        at = list(self.at)
        at[axis] = (at[axis] + step) % self.dims[axis]
        return tuple(at)

    def across(self, a, d):
        return ((self.at[0] + a) % self.dims[0], self.at[1], (self.at[2] + d) % self.dims[2])

    def back(self, offset):
        return tuple((p + n - o) % n for p, n, o in zip(self.at, self.dims, offset))

    def device(self, at):
        return (at[0] * 2 + self.core, at[1] * self.dims[2] + at[2])

    def partner(self):
        return (self.at[0] * 2 + 1 - self.core, lax.axis_index("sb"))

    def slot(self, at):
        return (at[0] * self.dims[1] + at[1]) * self.dims[2] + at[2]

    def greet(self):
        barrier = pltpu.get_barrier_semaphore()
        peers = [self.partner()]
        for axis in range(3):
            for step in range(1, self.dims[axis]):
                peers.append(self.device(self.other(axis, step)))
        for a in range(1, self.dims[0]):
            for d in range(1, self.dims[2]):
                peers.append(self.device(self.across(a, d)))
        for peer in peers:
            pl.semaphore_signal(barrier, inc=1, device_id=peer, device_id_type=MESH)
        pl.semaphore_wait(barrier, len(peers))


def pieces(x):
    hi = x.astype(BF)
    rest = x - hi.astype(F32)
    mid = rest.astype(BF)
    low = (rest - mid.astype(F32)).astype(BF)
    return hi, mid, low


def relay_lines(dims, b):
    na, nb, nd = dims
    sends = [((0, b, 0), 2, step) for step in range(1, nd)]
    return sends + [((0, b, 0), 0, step) for step in range(1, na)]


def relay_corners(dims, b):
    na, nb, nd = dims
    sends = [("q", (0, b, d), 0, s) for d in range(1, nd) for s in range(1, na)]
    return sends + [("d", (a, b, 0), 2, s) for a in range(1, na) for s in range(1, nd)]


def first_sends(dims):
    along = [(1, step) for step in range(1, dims[1])]
    across = [(2, step) for step in range(1, dims[2])] + [(0, step) for step in range(1, dims[0])]
    return along, across


def line_order(dims):
    lines = [(a, d) for a in range(dims[0]) for d in range(dims[2])]
    return sorted(lines, key=lambda at: (at[0] != 0) + (at[1] != 0))


def counts(dims):
    na, nb, nd = dims
    along, across = first_sends(dims)
    gathered = 4 * (len(along) + len(across))
    for b in range(nb):
        gathered += 2 * KVH * len(relay_lines(dims, b)) * (b > 0) + KVH * len(relay_corners(dims, b))
    lines = line_order(dims)
    reduced = sum((a != 0) + (d != 0) for a, d in lines) + (na - 1) + (nd - 1) + (nb - 1)
    return gathered, KVH * reduced, nb - 1 + na * nd - 1


def whole_kernel(dims, total_keys, tile, q_ref, d_ref, o_ref, lse_ref, k_ref, v_ref,
                 dq_out, dk_out, dv_out,
                 qa, da0, da1, kt, vt, ksend, krecv, auxs, qts, dts, ps, dss, dqs,
                 dk_acc, dv_acc, part, kvs, kvr,
                 r1a, r1b, t1a, t1b, r2a, r2b, t2, r3,
                 send_sem, q_sem, d_sem, kv_send, kv_recv, sum_send, sum_recv,
                 red_send, r1a_sem, r1b_sem, r2a_sem, r2b_sem, r3_sem):
    na, nb, nd = dims
    place = Place(dims)
    pa, pb, pd = place.at
    rows = q_ref.shape[0]
    keys = k_ref.shape[0]
    group = q_ref.shape[1] // KVH
    per_group = QH // KVH
    scale = 1.0 / math.sqrt(HEAD_DIM)
    along, across = first_sends(dims)
    origin = (0, 0, 0)
    block = nb * rows
    cols = block * per_group

    da1[pa, pb, pd] = d_ref[:, pl.ds(group, group)]
    for c in range(KVH):
        qa[c, pa, pb, pd] = q_ref[:, pl.ds(c * group, group)]
    chunk = 128

    def add_rows(n, total):
        at = pl.ds(pl.multiple_of(n * chunk, chunk), chunk)
        return total + jnp.sum(k_ref[at, :].astype(F32), axis=0, keepdims=True)

    key_sum = lax.fori_loop(0, keys // chunk, add_rows, jnp.zeros((1, KVH * HEAD_DIM), F32))
    row8 = lax.broadcasted_iota(jnp.int32, (8, HEAD_DIM), 0)
    sums = jnp.zeros((8, HEAD_DIM), F32)
    for c in range(KVH):
        sums = jnp.where(row8 == c, key_sum[:, c * HEAD_DIM:(c + 1) * HEAD_DIM], sums)
    ksend[0] = sums

    place.greet()

    partner_copies = []

    def to_partner(src, dst):
        n = len(partner_copies)
        copy = pltpu.make_async_remote_copy(
            src_ref=src, dst_ref=dst, send_sem=kv_send.at[n], recv_sem=kv_recv.at[n],
            device_id=place.partner(), device_id_type=MESH)
        copy.start()
        partner_copies.append(copy)
        return copy

    sum_copies = []

    def send_sums(stage, peers):
        group_of = []
        for peer in peers:
            n = len(sum_copies)
            copy = pltpu.make_async_remote_copy(
                src_ref=ksend.at[stage], dst_ref=krecv.at[n],
                send_sem=sum_send.at[n], recv_sem=sum_recv.at[n],
                device_id=place.device(peer), device_id_type=MESH)
            copy.start()
            sum_copies.append(copy)
            group_of.append((copy, n))
        return group_of

    def add_sums(stage, group_of):
        total = ksend[stage]
        for copy, n in group_of:
            copy.wait_recv()
            total = total + krecv[n]
        ksend[stage + 1] = total

    def flat(offset):
        return (offset[0] * nb + offset[1]) * nd + offset[2]

    def places(kind, at, offset):
        c = int(kind[1])
        if kind[0] == "q":
            return qa.at[c, at[0], at[1], at[2]], q_sem.at[c, flat(offset)]
        return (da0, da1)[c].at[at[0], at[1], at[2]], d_sem.at[c, flat(offset)]

    started = []

    def send(kind, offset, axis, step):
        there = list(offset)
        there[axis] = (there[axis] + step) % dims[axis]
        ref, sem = places(kind, place.back(offset), there)
        copy = pltpu.make_async_remote_copy(
            src_ref=ref, dst_ref=ref, send_sem=send_sem.at[len(started)], recv_sem=sem,
            device_id=place.device(place.other(axis, step)), device_id_type=MESH)
        copy.start()
        started.append(copy)

    arrived = set()

    def need(kind, offset):
        if offset == origin or (kind, offset) in arrived:
            return
        arrived.add((kind, offset))
        ref, sem = places(kind, place.back(offset), offset)
        pltpu.make_async_remote_copy(
            src_ref=ref, dst_ref=ref, send_sem=send_sem.at[0], recv_sem=sem,
            device_id=place.partner(), device_id_type=MESH).wait_recv()

    def send_first(kinds, directions):
        for kind in kinds:
            for axis, step in directions:
                send(kind, origin, axis, step)

    def send_line(c, b):
        for kind in ("q", "d"):
            need(kind + str(c), (0, b, 0))
        for kind in ("q", "d"):
            for offset, axis, step in relay_lines(dims, b):
                send(kind + str(c), offset, axis, step)

    def send_corner(c, b):
        for kind, offset, axis, step in relay_corners(dims, b):
            need(kind + str(c), offset)
            send(kind + str(c), offset, axis, step)

    def need_line(c, a, d):
        for b in range(nb):
            for kind in ("q", "d"):
                need(kind + str(c), (a, b, d))

    stage = send_sums(0, [place.other(1, step) for step in range(1, nb)])
    send_first(("q0",), along + across)
    lane = lax.broadcasted_iota(jnp.int32, (rows, HEAD_DIM), 1)
    lse_rows = lse_ref[...].T
    aux = jnp.zeros((rows, HEAD_DIM), F32)
    for head in range(QH):
        at = pl.ds(head * HEAD_DIM, HEAD_DIM)
        product = d_ref[:, at].astype(F32) * o_ref[:, at].astype(F32)
        delta = jnp.sum(product, axis=1, keepdims=True)
        offset = (lse_rows[:, head:head + 1] + math.log(total_keys)) * (1.0 / scale)
        for first, value in ((0, offset), (3 * QH, delta)):
            for n, piece in enumerate(pieces(value)):
                aux = jnp.where(lane == first + 3 * head + n, piece.astype(F32), aux)
    da0[pa, pb, pd, :, pl.ds(group, HEAD_DIM)] = aux.astype(BF)
    da0[pa, pb, pd, :, pl.ds(0, group)] = d_ref[:, pl.ds(0, group)]
    send_first(("d0",), along + across)

    def turn(n, carry):
        at = pl.ds(pl.multiple_of(n * chunk, chunk), chunk)
        for c in range(KVH):
            head = pl.ds(c * HEAD_DIM, HEAD_DIM)
            kt[0, c, :, at] = k_ref[at, head].T
            vt[0, c, :, at] = v_ref[at, head].T
        return carry

    lax.fori_loop(0, keys // chunk, turn, 0)
    k_copy = to_partner(kt.at[0], kt.at[1])
    v_copy = to_partner(vt.at[0], vt.at[1])
    add_sums(0, stage)
    stage = send_sums(1, [place.across(a, d) for a, d in line_order(dims)[1:]])
    send_first(("q1", "d1"), across)
    send_corner(0, 0)
    add_sums(1, stage)
    sum_copy = to_partner(ksend.at[2], ksend.at[3])
    for b in range(1, nb):
        send_line(0, b)
    send_first(("q1", "d1"), along)
    k_copy.wait_recv()
    v_copy.wait_recv()
    sum_copy.wait_recv()
    k_copy.wait_send()
    mean = (ksend[2] + ksend[3]) * (1.0 / total_keys)

    def smooth(c):
        mean_t = jnp.broadcast_to(mean[c:c + 1], (HEAD_DIM, HEAD_DIM)).T

        def part_of(n, carry):
            at = pl.ds(pl.multiple_of(n * chunk, chunk), chunk)
            for side in range(2):
                kt[side, c, :, at] = (kt[side, c, :, at].astype(F32) - mean_t).astype(BF)
            return carry

        lax.fori_loop(0, keys // chunk, part_of, 0)

    nt = (((1,), (1,)), ((), ()))
    tiles = keys // tile
    lane_b = lax.broadcasted_iota(jnp.int32, (block, HEAD_DIM), 1)

    def line_at(a, d):
        return (pa + na - a) % na, (pd + nd - d) % nd

    def prepare(n, c, a, d):
        la, ld = line_at(a, d)
        aux_rows = da0[la, :, ld, :, pl.ds(group, HEAD_DIM)].reshape(block, HEAD_DIM)
        for g in range(per_group):
            head = pl.ds(g * HEAD_DIM, HEAD_DIM)
            here = pl.ds(g * block, block)
            low = 3 * (c * per_group + g)
            keep = (lane_b >= low) & (lane_b < low + 3)
            low = low + 3 * QH
            keep = keep | ((lane_b >= low) & (lane_b < low + 3))
            auxs[n, here, :] = jnp.where(keep, aux_rows.astype(F32), 0.0).astype(BF)
            qts[n, :, here] = qa[c, la, :, ld, :, head].reshape(block, HEAD_DIM).T
            dts[n, :, here] = (da0, da1)[c][la, :, ld, :, head].reshape(block, HEAD_DIM).T

    def scores(n, m, c, a, d, side, t):
        la, ld = line_at(a, d)
        at = pl.ds(t * tile, tile)
        key_row = lax.broadcasted_iota(jnp.int32, (HEAD_DIM, tile), 0)
        pick_s = jnp.where(key_row < 3 * QH, -1.0, 0.0).astype(BF)
        pick_d = jnp.where((key_row >= 3 * QH) & (key_row < 6 * QH), -1.0, 0.0).astype(BF)
        kk = jnp.concatenate([kt[side, c, :, at], pick_s], 0)
        vv = jnp.concatenate([vt[side, c, :, at], pick_d], 0)
        for g in range(per_group):
            head = pl.ds(g * HEAD_DIM, HEAD_DIM)
            here = pl.ds(g * block, block)
            qh = qa[c, la, :, ld, :, head].reshape(block, HEAD_DIM)
            dh = (da0, da1)[c][la, :, ld, :, head].reshape(block, HEAD_DIM)
            s = jnp.dot(jnp.concatenate([qh, auxs[n, here, :]], 1), kk, preferred_element_type=F32)
            dp = jnp.dot(jnp.concatenate([dh, auxs[n, here, :]], 1), vv, preferred_element_type=F32)
            prob = jnp.exp2(s * (scale * math.log2(math.e)))
            ps[m, here, :] = prob.astype(BF)
            dss[m, here, :] = (prob * dp).astype(BF)

    def products(n, m, c, side, t, first_line, first_tile):
        at = pl.ds(t * tile, tile)
        dv = jnp.dot(dts[n], ps[m], preferred_element_type=F32)
        dk = jnp.dot(qts[n], dss[m], preferred_element_type=F32)
        dq = lax.dot_general(kt[side, c, :, at], dss[m], nt, preferred_element_type=F32)
        if first_line:
            dv_acc[side, c, :, at] = dv
            dk_acc[side, c, :, at] = dk
        else:
            dv_acc[side, c, :, at] += dv
            dk_acc[side, c, :, at] += dk
        if first_tile:
            dqs[n] = dq
        else:
            dqs[n] += dq

    def finish(n, c, a, d):
        la, ld = line_at(a, d)
        for g in range(per_group):
            here = pl.ds(g * block, block)
            piece = (dqs[n, :, here] * scale).astype(BF).T
            part[c, la, :, ld, :, pl.ds(g * HEAD_DIM, HEAD_DIM)] = piece.reshape(nb, rows, HEAD_DIM)

    mid = group // 2
    left, right = pl.ds(0, mid), pl.ds(mid, mid)
    reduced = []

    def red(src, dst, sem, to):
        copy = pltpu.make_async_remote_copy(
            src_ref=src, dst_ref=dst, send_sem=red_send.at[len(reduced)], recv_sem=sem,
            device_id=place.device(to), device_id_type=MESH)
        copy.start()
        reduced.append(copy)

    def landed(ref, sem):
        pltpu.make_async_remote_copy(
            src_ref=ref, dst_ref=ref, send_sem=red_send.at[0], recv_sem=sem,
            device_id=place.partner(), device_id_type=MESH).wait_recv()

    def stage1(c, a, d):
        la, ld = line_at(a, d)
        if d:
            s = nd - d
            red(part.at[c, la, :, ld, :, left], r1a.at[c, s - 1, la],
                r1a_sem.at[c, s - 1, a], place.other(2, s))
        if a:
            s = na - a
            red(part.at[c, la, :, ld, :, right], r1b.at[c, s - 1, ld],
                r1b_sem.at[c, s - 1, d], place.other(0, s))

    def sum_left(c, a):
        la, _ = line_at(a, 0)
        total = part[c, la, :, pd, :, left].astype(F32)
        for s in range(nd - 1):
            landed(r1a.at[c, s, la], r1a_sem.at[c, s, a])
            total = total + r1a[c, s, la].astype(F32)
        return total

    def sum_right(c, d):
        _, ld = line_at(0, d)
        total = part[c, pa, :, ld, :, right].astype(F32)
        for s in range(na - 1):
            landed(r1b.at[c, s, ld], r1b_sem.at[c, s, d])
            total = total + r1b[c, s, ld].astype(F32)
        return total

    def stage2(c):
        for a in range(1, na):
            t1a[c, a] = sum_left(c, a).astype(BF)
            s = na - a
            red(t1a.at[c, a], r2a.at[c, s - 1], r2a_sem.at[c, s - 1], place.other(0, s))
        for d in range(1, nd):
            t1b[c, d] = sum_right(c, d).astype(BF)
            s = nd - d
            red(t1b.at[c, d], r2b.at[c, s - 1], r2b_sem.at[c, s - 1], place.other(2, s))

    def stage3(c):
        total = sum_left(c, 0)
        for s in range(na - 1):
            landed(r2a.at[c, s], r2a_sem.at[c, s])
            total = total + r2a[c, s].astype(F32)
        t2[c, :, :, left] = total.astype(BF)
        total = sum_right(c, 0)
        for s in range(nd - 1):
            landed(r2b.at[c, s], r2b_sem.at[c, s])
            total = total + r2b[c, s].astype(F32)
        t2[c, :, :, right] = total.astype(BF)
        for s in range(1, nb):
            to = place.other(1, s)
            red(t2.at[c, to[1]], r3.at[c, s - 1], r3_sem.at[c, s - 1], to)

    def last(c):
        total = t2[c, pb].astype(F32)
        for s in range(nb - 1):
            landed(r3.at[c, s], r3_sem.at[c, s])
            total = total + r3[c, s].astype(F32)
        dq_out[:, pl.ds(c * group, group)] = total

    kv = []

    def share(c):
        for which, acc, factor in ((0, dk_acc, scale), (1, dv_acc, 1.0)):
            kvs[c, which] = (acc[1, c] * factor).astype(BF)
            kv.append(to_partner(kvs.at[c, which], kvr.at[c, which]))

    def collect(c):
        head = pl.ds(c * HEAD_DIM, HEAD_DIM)
        for which, acc, factor, out in ((0, dk_acc, scale, dk_out), (1, dv_acc, 1.0, dv_out)):
            kv[2 * c + which].wait_recv()
            total = acc[0, c] * factor + kvr[c, which].astype(F32)
            out[:, head] = total.astype(BF).T

    lines = line_order(dims)
    far = [at for at in lines if at[0] and at[1]]
    straight = [at for at in lines if bool(at[0]) != bool(at[1])]
    near_y = [at for at in straight if at[0]]
    near_x = [at for at in straight if at[1]]
    orders = (lines, near_y + far + near_x + lines[:1])
    events = {}
    half = len(lines) * 2 * tiles

    def plan(k, action, *args):
        events.setdefault(k * half // 16, []).append(functools.partial(action, *args))

    for b in range(1, nb):
        plan(min(b + 1, 4), send_corner, 0, b)
        plan(min(6 + 3 * b, 15), send_line, 1, b)
    for b in range(nb):
        plan(5 if b == 0 else min(13 + 2 * b, 18), send_corner, 1, b)
    for n, (a, d) in enumerate(lines[1:]):
        plan(min(19 + n, 22), stage1, 0, a, d)
    plan(28, stage2, 0)
    plan(30, stage2, 1)

    steps = [(side, t) for side in (1, 0) for t in range(tiles)]
    pending = ended = None
    count = 0
    for c in range(KVH):
        smooth(c)
        for n, (a, d) in enumerate(orders[c]):
            slot = n % 2
            for i, (side, t) in enumerate(steps):
                for action in events.get(count, []):
                    action()
                if i == 0:
                    need_line(c, a, d)
                    need_line(0, a, d)
                    prepare(slot, c, a, d)
                scores(slot, count % 2, c, a, d, side, t)
                if pending is not None:
                    products(*pending)
                if ended is not None:
                    finish(*ended)
                    if c:
                        stage1(*ended[1:])
                pending = (slot, count % 2, c, side, t, n == 0, i == 0)
                ended = None
                count += 1
            ended = (slot, c, a, d)
        products(*pending)
        finish(*ended)
        pending = ended = None
        share(c)
    stage3(0)
    stage3(1)
    collect(0)
    last(0)
    collect(1)
    last(1)
    for copy in started + partner_copies[1:] + sum_copies + reduced:
        copy.wait_send()


def local(dims, q, d, o, lse, k, v):
    na, nb, nd = dims
    members = na * nb * nd
    rows, width = q.shape
    keys, kw = k.shape
    group, mid = width // KVH, width // KVH // 2
    cols = nb * rows * (QH // KVH)
    tile = min(512, keys)
    gathered, reduced, summed = counts(dims)
    vmem = pl.BlockSpec(memory_space=pltpu.VMEM)
    ma, mb, md = max(na - 1, 1), max(nb - 1, 1), max(nd - 1, 1)
    sem = pltpu.SemaphoreType.DMA
    return pl.pallas_call(
        functools.partial(whole_kernel, dims, keys * members * 2, tile),
        name="whole",
        out_shape=(
            jax.ShapeDtypeStruct((rows, width), F32),
            jax.ShapeDtypeStruct((keys, kw), BF),
            jax.ShapeDtypeStruct((keys, kw), BF),
        ),
        in_specs=[vmem] * 6,
        out_specs=(vmem,) * 3,
        scratch_shapes=[
            pltpu.VMEM((KVH, na, nb, nd, rows, group), BF),
            pltpu.VMEM((na, nb, nd, rows, group + HEAD_DIM), BF),
            pltpu.VMEM((na, nb, nd, rows, group), BF),
            pltpu.VMEM((2, KVH, HEAD_DIM, keys), BF),
            pltpu.VMEM((2, KVH, HEAD_DIM, keys), BF),
            pltpu.VMEM((4, 8, HEAD_DIM), F32),
            pltpu.VMEM((max(summed, 1), 8, HEAD_DIM), F32),
            pltpu.VMEM((2, cols, HEAD_DIM), BF),
            pltpu.VMEM((2, HEAD_DIM, cols), BF),
            pltpu.VMEM((2, HEAD_DIM, cols), BF),
            pltpu.VMEM((2, cols, tile), BF),
            pltpu.VMEM((2, cols, tile), BF),
            pltpu.VMEM((2, HEAD_DIM, cols), F32),
            pltpu.VMEM((2, KVH, HEAD_DIM, keys), F32),
            pltpu.VMEM((2, KVH, HEAD_DIM, keys), F32),
            pltpu.VMEM((KVH, na, nb, nd, rows, group), BF),
            pltpu.VMEM((KVH, 2, HEAD_DIM, keys), BF),
            pltpu.VMEM((KVH, 2, HEAD_DIM, keys), BF),
            pltpu.VMEM((KVH, md, na, nb, rows, mid), BF),
            pltpu.VMEM((KVH, ma, nd, nb, rows, mid), BF),
            pltpu.VMEM((KVH, na, nb, rows, mid), BF),
            pltpu.VMEM((KVH, nd, nb, rows, mid), BF),
            pltpu.VMEM((KVH, ma, nb, rows, mid), BF),
            pltpu.VMEM((KVH, md, nb, rows, mid), BF),
            pltpu.VMEM((KVH, nb, rows, group), BF),
            pltpu.VMEM((KVH, mb, rows, group), BF),
            sem((gathered,)),
            sem((KVH, members)),
            sem((KVH, members)),
            sem((3 + 2 * KVH,)),
            sem((3 + 2 * KVH,)),
            sem((max(summed, 1),)),
            sem((max(summed, 1),)),
            sem((reduced,)),
            sem((KVH, md, na)),
            sem((KVH, ma, nd)),
            sem((KVH, ma)),
            sem((KVH, md)),
            sem((KVH, mb)),
        ],
        compiler_params=pltpu.CompilerParams(
            collective_id=0, has_side_effects=True, vmem_limit_bytes=60 * 1024 * 1024),
    )(q, d, o, lse.T, k, v)


def solution(mesh):
    dims = grid_of(mesh.shape["sa"], mesh.shape["sb"])
    spec = P(("sa", "sb"), None)
    return jax.shard_map(functools.partial(local, dims), mesh=mesh, in_specs=(spec,) * 6,
                         out_specs=(spec,) * 3, check_vma=False)
```
